32 devices in a mesh: row: 4 (over x, core), col: 8 (over z, y).
Axes of the slice: x: 2, y: 2, z: 4, core: 2. Of those that a mesh axis runs over, the one named last changes fastest.
Arguments:
- momentum: float32 [5120, 27648], P('row', 'col'), may hold values from -130 to 130, as said below
- activations: bfloat16 [2048, 5120], P(None, 'row'), may hold values from -6 to 6
- out_grads: bfloat16 [2048, 27648], P(None, 'col'), may hold values from -0.125 to 0.125
- basis: float32 [27648, 256], P('col'), may hold values from -6 to 6
Outputs:
- new_momentum: float32 [5120, 27648], P('row', 'col')
- left_basis: float32 [5120, 256], P('row')
- new_basis: float32 [27648, 256], P('col')
The draws below stay inside these ranges and needn't reach their ends.
Inputs may be any that keep to these rules, and one draw needn't show every extreme that they name: `momentum`: Real-valued entries of order one with varying row and column scales.
All inputs are finite; a program needn't handle non-finite values.
Results may differ from the reference program's by a relative error of at most 0.0003.
Values sent between devices are 32-bit elements; how exact they have to be, the bound alone decides.
No kernel may reach another device: no remote copies, remote signals or barrier semaphores. Data moves between devices by JAX's collectives and lax.ppermute only.
A program may use at most 128 MiB of HBM per device.

```python
import math
import jax
import jax.numpy as jnp
from jax import lax

D = 5120
F = 27648
RANK = 256
TOKENS = 2048


def draw_momentum(key, part):
    keys = jax.random.split(jax.random.fold_in(key, 11), 3)
    row_pos = jnp.arange(D, dtype=jnp.float32) / D
    col_pos = jnp.arange(F, dtype=jnp.float32) / F
    trend_rows = jnp.exp(0.5 * math.log(3.0) * (row_pos - 0.5))
    trend_cols = jnp.exp(0.5 * math.log(3.0) * (col_pos - 0.5))
    base = jax.random.truncated_normal(keys[0], -4.0, 4.0, (D, F), jnp.float32)
    row_scale = jnp.exp(jax.random.uniform(keys[1], (D,), jnp.float32, math.log(0.3), math.log(3.0))) * trend_rows
    col_scale = jnp.exp(jax.random.uniform(keys[2], (F,), jnp.float32, math.log(0.3), math.log(3.0))) * trend_cols
    return base * row_scale[:, None] * col_scale[None, :]


def shard_levels(rng, extent, pieces, low, high):
    gain, own = 1.0, jax.random.fold_in(rng, 6)
    for axis_at, shards_of in pieces:
        draws = jnp.exp(jax.random.uniform(jax.random.fold_in(own, axis_at), (shards_of,), jnp.float32, low / len(pieces), high / len(pieces)))
        gain = gain * jnp.repeat(draws, extent[axis_at] // shards_of).reshape([-1 if axis == axis_at else 1 for axis in range(len(extent))])
    return gain


def bell_draw(rng, dims, scale, most, cuts=(), kind=jnp.bfloat16):
    level = shard_levels(rng, dims, cuts, -0.22, 0.18) if cuts else 1.0
    array = jax.random.normal(rng, dims, jnp.float32) * scale * level
    return jnp.minimum(jnp.maximum(array, -most), most).astype(kind)


def setup_inputs(seed: int = 0) -> dict:
    seeds = jax.random.split(jax.random.key(seed), 5)
    momentum = draw_momentum(jax.random.fold_in(seeds[4], 71), 0)
    activations = bell_draw(seeds[1], (TOKENS, D), 1.0, 6.0, ((1, 4),))
    out_grads = bell_draw(seeds[2], (TOKENS, F), TOKENS ** -0.5, 0.125, ((1, 8),))
    basis = bell_draw(seeds[3], (F, RANK), 1.0, 6.0, ((0, 8),), jnp.float32)
    return dict(momentum=momentum, activations=activations, out_grads=out_grads, basis=basis)


EPS = 1e-06
HIGH = lax.Precision.HIGHEST

def reference(momentum, activations, out_grads, basis):
    gradient = lax.dot_general(activations.astype(jnp.float32), out_grads.astype(jnp.float32), (((0,), (0,)), ((), ())), preferred_element_type=jnp.float32)
    merged = momentum + gradient
    projected = jnp.dot(merged, basis, precision=HIGH)
    gram_total = jnp.dot(projected.T, projected, precision=HIGH)
    factor = jnp.linalg.cholesky(gram_total)
    ortho = jax.scipy.linalg.solve_triangular(factor, projected.T, lower=True).T
    coeffs = jnp.dot(merged.T, ortho, precision=HIGH)
    new_momentum = merged - 0.5 * jnp.dot(ortho, coeffs.T, precision=HIGH)
    inv_norm = lax.rsqrt(lax.optimization_barrier(jnp.mean(coeffs * coeffs, axis=0)) + EPS)
    return (new_momentum, ortho * jnp.float32(math.sqrt(D)), coeffs * inv_norm[None, :])
```

```python
import math

import jax
import jax.numpy as jnp
from jax import lax
from jax.experimental import pallas as pl
from jax.experimental.pallas import tpu as pltpu
from jax.sharding import PartitionSpec as P


EPS = 1e-06
HIGH = lax.Precision.HIGHEST
F32 = jnp.float32
BF16 = jnp.bfloat16
LANES = 128
NN = (((1,), (0,)), ((), ()))
NT = (((1,), (1,)), ((), ()))


def split(x):
    hi = x.astype(BF16)
    return hi, (x - hi.astype(F32)).astype(BF16)


def dot(a, b, dims=NN):
    return lax.dot_general(a, b, dims, preferred_element_type=F32)


def params(flops, **kw):
    return dict(
        compiler_params=pltpu.CompilerParams(vmem_limit_bytes=56 * 2**20, **kw),
        cost_estimate=pl.CostEstimate(flops=flops, transcendentals=0, bytes_accessed=flops // 300),
    )


WIDE = 512


def joined3(left):
    return jnp.concatenate([left[0], left[1], left[0]], axis=1)


def front_kernel(momentum, activations, out_grads, basis, pieces):
    rows, cols = momentum.shape
    tokens, rank = out_grads.shape[0], basis.shape[1]
    high = rows // pieces
    wide = min(WIDE, cols)
    steps = pl.cdiv(cols, wide)
    last = cols - (steps - 1) * wide

    def body(mom_ref, act_ref, grad_ref, basis_ref, merged_ref, *rest):
        proj_refs, act_t = rest[:-1], rest[-1]
        step = pl.program_id(0)

        @pl.when(step == 0)
        def _():
            act_t[...] = act_ref[...].T
            for proj_ref in proj_refs:
                proj_ref[...] = jnp.zeros_like(proj_ref)

        def block(width):
            b_hi, b_lo = split(basis_ref[:width, :])
            right = jnp.concatenate([b_hi, b_hi, b_lo], axis=0)
            for k, proj_ref in enumerate(proj_refs):
                at = slice(k * high, (k + 1) * high)
                merged = mom_ref[at, :width] + dot(act_t[at, :], grad_ref[:, :width])
                merged_ref[at, :width] = merged
                proj_ref[...] += dot(joined3(split(merged)), right)

        if last == wide:
            block(wide)
        else:
            pl.when(step < steps - 1)(lambda: block(wide))
            pl.when(step == steps - 1)(lambda: block(last))

    return pl.pallas_call(
        body,
        grid=(steps,),
        in_specs=[
            pl.BlockSpec((rows, wide), lambda j: (0, j)),
            pl.BlockSpec((tokens, rows), lambda j: (0, 0)),
            pl.BlockSpec((tokens, wide), lambda j: (0, j)),
            pl.BlockSpec((wide, rank), lambda j: (j, 0)),
        ],
        out_specs=[pl.BlockSpec((rows, wide), lambda j: (0, j))]
        + [pl.BlockSpec((high, rank), lambda j: (0, 0))] * pieces,
        out_shape=[jax.ShapeDtypeStruct((rows, cols), F32)]
        + [jax.ShapeDtypeStruct((high, rank), F32)] * pieces,
        scratch_shapes=[pltpu.VMEM((rows, tokens), BF16)],
        name="front",
        **params(2 * rows * cols * (tokens + 3 * rank)),
    )(momentum, activations, out_grads, basis)


def gram_kernel(projected):
    rows, rank = projected.shape

    def body(proj_ref, gram_ref, turned_ref):
        value = proj_ref[...]
        hi, lo = split(value)
        t_hi, t_lo = hi.T, lo.T
        turned_ref[:rank, :] = t_hi
        turned_ref[rank:, :] = t_lo
        gram_ref[...] = dot(joined3((t_hi, t_lo)), jnp.concatenate([hi, hi, lo], axis=0))

    return pl.pallas_call(
        body,
        out_shape=[
            jax.ShapeDtypeStruct((rank, rank), F32),
            jax.ShapeDtypeStruct((2 * rank, rows), BF16),
        ],
        name="gram",
        **params(6 * rows * rank * rank),
    )(projected)


def right_kernel(merged, turned, start, span):
    rows = merged.shape[0]
    rank = turned.shape[0] // 2
    wide = min(WIDE, span)
    first = start // wide

    def body(merged_ref, turned_ref, out_ref):
        hi, lo = split(merged_ref[...])
        total = dot(turned_ref[...], hi)
        out_ref[...] = (total[:rank] + total[rank:] + dot(turned_ref[:rank, :], lo)).T

    return pl.pallas_call(
        body,
        grid=(pl.cdiv(span, wide),),
        in_specs=[
            pl.BlockSpec((rows, wide), lambda j: (0, first + j)),
            pl.BlockSpec((2 * rank, rows), lambda j: (0, 0)),
        ],
        out_specs=pl.BlockSpec((wide, rank), lambda j: (j, 0)),
        out_shape=jax.ShapeDtypeStruct((span, rank), F32),
        name="right",
        **params(6 * rows * span * rank),
    )(merged, turned)


def invert_base(block):
    size = block.shape[0]
    rows = [block[8 * g : 8 * g + 8, :] for g in range(size // 8)]
    lane = lax.broadcasted_iota(jnp.int32, (8, size), 1)
    sub = lax.broadcasted_iota(jnp.int32, (8, size), 0)
    for j in range(size):
        home, s = divmod(j, 8)
        column = jnp.broadcast_to(rows[home][:, j : j + 1], (8, size))
        pivot_row = rows[home][s : s + 1, :] / column[s : s + 1, :]
        pivot_inv = 1.0 / column[s : s + 1, :]
        here = lane == j
        pivot_row = jnp.broadcast_to(pivot_row, (8, size))
        pivot_inv = jnp.broadcast_to(pivot_inv, (8, size))
        for g in range(home, size // 8):
            if g > home:
                column = jnp.broadcast_to(rows[g][:, j : j + 1], (8, size))
            new = jnp.where(here, -column * pivot_inv, rows[g] - column * pivot_row)
            rows[g] = jnp.where(sub > s, new, rows[g]) if g == home else new
    out = []
    for g in range(size // 8):
        diagonal = lane == sub + 8 * g
        pivots = jnp.sum(jnp.where(diagonal, rows[g], 0.0), axis=1, keepdims=True)
        scale = 1.0 / jnp.sqrt(pivots)
        unit = jnp.where(lane < sub + 8 * g, rows[g], jnp.where(diagonal, 1.0, 0.0))
        out.append(unit * scale)
    return jnp.concatenate(out, axis=0)


def full_dot(a, b, dims=NN):
    return lax.dot_general(a, b, dims, precision=HIGH, preferred_element_type=F32)


def invert_factor(gram):
    size = gram.shape[0]
    if size <= LANES:
        return invert_base(gram)
    half = size // 2
    first = invert_factor(gram[:half, :half])
    below = full_dot(gram[half:, :half], first, NT)
    second = invert_factor(gram[half:, half:] - full_dot(below, below, NT))
    corner = -full_dot(second, full_dot(below, first))
    top = jnp.concatenate([first, jnp.zeros((half, size - half), F32)], axis=1)
    return jnp.concatenate([top, jnp.concatenate([corner, second], axis=1)], axis=0)


def ortho_kernel(gram, projected, root):
    rows, rank = projected.shape

    def body(gram_ref, proj_ref, inv_ref, left_ref, wide_ref):
        inverse = invert_factor(gram_ref[...])
        inv_ref[...] = inverse
        i_hi, i_lo = split(inverse)
        ortho = dot(joined3(split(proj_ref[...])), jnp.concatenate([i_hi, i_hi, i_lo], axis=1), NT)
        left_ref[...] = ortho * root
        wide_ref[...] = joined3(split(ortho))

    return pl.pallas_call(
        body,
        out_shape=[
            jax.ShapeDtypeStruct((rank, rank), F32),
            jax.ShapeDtypeStruct((rows, rank), F32),
            jax.ShapeDtypeStruct((rows, 3 * rank), BF16),
        ],
        name="ortho",
        **params(40 * 10**9),
    )(gram, projected)


def coeff_kernel(right, inverse):
    rows, rank = right.shape

    def body(right_ref, inv_ref, out_ref, sq_ref):
        i_hi, i_lo = split(inv_ref[...])
        coeffs = dot(joined3(split(right_ref[...])), jnp.concatenate([i_hi, i_hi, i_lo], axis=1), NT)
        out_ref[...] = coeffs
        sq_ref[...] = jnp.sum(coeffs * coeffs, axis=0, keepdims=True)

    return pl.pallas_call(
        body,
        out_shape=[jax.ShapeDtypeStruct((rows, rank), F32), jax.ShapeDtypeStruct((1, rank), F32)],
        name="coeff",
        **params(6 * rows * rank * rank),
    )(right, inverse)


def update_kernel(merged, wide_ortho, coeffs):
    rows, cols = merged.shape
    rank = coeffs[0].shape[1]
    wide = min(WIDE, cols)
    counts = [pl.cdiv(c.shape[0], wide) for c in coeffs]
    starts = [sum(counts[:k]) for k in range(len(counts))]
    chunks = len(coeffs)

    def body(ortho_ref, merged_ref, *rest):
        out_ref, turned_ref = rest[-2:]
        step = pl.program_id(0)
        for k in range(chunks):

            @pl.when((step >= starts[k]) & (step < starts[k] + counts[k]))
            def _(k=k):
                c_hi, c_lo = split(rest[k][...] * -0.5)
                turned_ref[...] = jnp.concatenate([c_hi, c_hi, c_lo], axis=1)

        out_ref[...] = merged_ref[...] + dot(ortho_ref[...], turned_ref[...], NT)

    def at(k):
        return lambda j: (jnp.clip(j - starts[k], 0, counts[k] - 1), 0)

    return pl.pallas_call(
        body,
        grid=(sum(counts),),
        in_specs=[
            pl.BlockSpec((rows, 3 * rank), lambda j: (0, 0)),
            pl.BlockSpec((rows, wide), lambda j: (0, j)),
        ]
        + [pl.BlockSpec((wide, rank), at(k)) for k in range(chunks)],
        out_specs=pl.BlockSpec((rows, wide), lambda j: (0, j)),
        out_shape=jax.ShapeDtypeStruct((rows, cols), F32),
        scratch_shapes=[pltpu.VMEM((wide, 3 * rank), BF16)],
        name="update",
        **params(6 * rows * cols * rank),
    )(wide_ortho, merged, *coeffs)


def swap(x, axis, size, bit):
    return lax.ppermute(x, axis, [(i, i ^ (1 << bit)) for i in range(size)])


def bits_of(size):
    bits = size.bit_length() - 1
    return bits if size == 1 << bits else None


def keep_and_send(x, mine):
    half = x.shape[0] // 2
    keep = lax.dynamic_slice_in_dim(x, mine * half, half, 0)
    send = lax.dynamic_slice_in_dim(x, (1 - mine) * half, half, 0)
    return keep, send


def join(own, other, mine):
    return jnp.where(mine == 0, jnp.concatenate([own, other], 0), jnp.concatenate([other, own], 0))


def reduce_all(x, axis, size, halved):
    bits = bits_of(size)
    if bits is None or x.shape[0] % (1 << len(halved)):
        return lax.psum(x, axis)
    at = lax.axis_index(axis)
    for bit in halved:
        keep, send = keep_and_send(x, (at >> bit) & 1)
        x = keep + swap(send, axis, size, bit)
    for bit in range(bits):
        if bit not in halved:
            x = x + swap(x, axis, size, bit)
    for bit in reversed(halved):
        x = join(x, swap(x, axis, size, bit), (at >> bit) & 1)
    return x


def solution(mesh):
    n_row, n_col = mesh.shape["row"], mesh.shape["col"]
    col_halved = list(range((bits_of(n_col) or 0) - 1))

    def spans_of(cols):
        return [2 * WIDE, 3 * WIDE, cols - 5 * WIDE] if cols > 6 * WIDE else [cols]

    def shards(momentum, activations, out_grads, basis):
        rows, cols = momentum.shape
        spans = spans_of(cols)
        merged, *parts = front_kernel(momentum, activations, out_grads, basis, 2)
        parts = [reduce_all(p, "col", n_col, col_halved) for p in parts]
        projected = jnp.concatenate(parts, axis=0)
        gram_part, turned = gram_kernel(projected)
        gram = reduce_all(gram_part, "row", n_row, [0])
        rights = []
        for k, span in enumerate(spans):
            part = right_kernel(merged, turned, sum(spans[:k]), span)
            rights.append(reduce_all(part, "row", n_row, [0]))
        inverse, left_basis, wide_ortho = ortho_kernel(gram, projected, math.sqrt(rows * n_row))
        pairs = [coeff_kernel(r, inverse) for r in rights]
        coeffs = [c for c, _ in pairs]
        squares = reduce_all(sum(s for _, s in pairs), "col", n_col, [])
        new_momentum = update_kernel(merged, wide_ortho, coeffs)
        inv_norm = lax.rsqrt(squares / (cols * n_col) + EPS)
        new_basis = jnp.concatenate([c * inv_norm for c in coeffs], axis=0)
        return new_momentum, left_basis, new_basis

    return jax.shard_map(
        shards,
        mesh=mesh,
        in_specs=(P("row", "col"), P(None, "row"), P(None, "col"), P("col", None)),
        out_specs=(P("row", "col"), P("row", None), P("col", None)),
        check_vma=False,
    )
```

```python
import math

import jax
import jax.numpy as jnp
from jax import lax
from jax.experimental import pallas as pl
from jax.experimental.pallas import tpu as pltpu
from jax.sharding import PartitionSpec as P


EPS = 1e-06
HIGH = lax.Precision.HIGHEST
F32 = jnp.float32
BF16 = jnp.bfloat16
LANES = 128
NN = (((1,), (0,)), ((), ()))
NT = (((1,), (1,)), ((), ()))


def split(x):
    hi = x.astype(BF16)
    return hi, (x - hi.astype(F32)).astype(BF16)


def dot(a, b, dims=NN):
    return lax.dot_general(a, b, dims, preferred_element_type=F32)


def params(flops, room=20, **kw):
    return dict(
        compiler_params=pltpu.CompilerParams(vmem_limit_bytes=room * 2**20, **kw),
        cost_estimate=pl.CostEstimate(flops=flops, transcendentals=0, bytes_accessed=flops // 300),
    )


WIDE = 512


def joined3(left):
    return jnp.concatenate([left[0], left[1], left[0]], axis=1)


def front_kernel(momentum, activations, out_grads, basis, pieces):
    rows, cols = momentum.shape
    tokens, rank = out_grads.shape[0], basis.shape[1]
    high = rows // pieces
    wide = min(WIDE, cols)
    steps = pl.cdiv(cols, wide)
    last = cols - (steps - 1) * wide

    def body(mom_ref, act_ref, grad_ref, basis_ref, merged_ref, *rest):
        proj_refs, act_t = rest[:-1], rest[-1]
        step = pl.program_id(0)

        @pl.when(step == 0)
        def _():
            act_t[...] = act_ref[...].T
            for proj_ref in proj_refs:
                proj_ref[...] = jnp.zeros_like(proj_ref)

        def block(width):
            b_hi, b_lo = split(basis_ref[:width, :])
            right = jnp.concatenate([b_hi, b_hi, b_lo], axis=0)
            for k, proj_ref in enumerate(proj_refs):
                at = slice(k * high, (k + 1) * high)
                merged = mom_ref[at, :width] + dot(act_t[at, :], grad_ref[:, :width])
                merged_ref[at, pl.ds(pl.multiple_of(step * wide, wide), width)] = merged
                proj_ref[...] += dot(joined3(split(merged)), right)

        if last == wide:
            block(wide)
        else:
            pl.when(step < steps - 1)(lambda: block(wide))
            pl.when(step == steps - 1)(lambda: block(last))

    return pl.pallas_call(
        body,
        grid=(steps,),
        in_specs=[
            pl.BlockSpec((rows, wide), lambda j: (0, j)),
            pl.BlockSpec((tokens, rows), lambda j: (0, 0)),
            pl.BlockSpec((tokens, wide), lambda j: (0, j)),
            pl.BlockSpec((wide, rank), lambda j: (j, 0)),
        ],
        out_specs=[pl.BlockSpec(memory_space=pltpu.VMEM)]
        + [pl.BlockSpec((high, rank), lambda j: (0, 0))] * pieces,
        out_shape=[pltpu.VMEM((rows, cols), F32)]
        + [jax.ShapeDtypeStruct((high, rank), F32)] * pieces,
        scratch_shapes=[pltpu.VMEM((rows, tokens), BF16)],
        name="front",
        **params(2 * rows * cols * (tokens + 3 * rank), 40),
    )(momentum, activations, out_grads, basis)


def gram_kernel(projected):
    rows, rank = projected.shape

    def body(proj_ref, gram_ref, turned_ref):
        value = proj_ref[...]
        hi, lo = split(value)
        t_hi, t_lo = hi.T, lo.T
        turned_ref[:rank, :] = t_hi
        turned_ref[rank:, :] = t_lo
        gram_ref[...] = dot(joined3((t_hi, t_lo)), jnp.concatenate([hi, hi, lo], axis=0))

    return pl.pallas_call(
        body,
        out_shape=[
            jax.ShapeDtypeStruct((rank, rank), F32),
            jax.ShapeDtypeStruct((2 * rank, rows), BF16),
        ],
        name="gram",
        **params(6 * rows * rank * rank),
    )(projected)


def right_kernel(merged, turned, start, span):
    rows = merged.shape[0]
    rank = turned.shape[0] // 2
    wide = min(WIDE, span)

    def body(merged_ref, turned_ref, out_ref):
        for at in range(0, span, wide):
            width = min(wide, span - at)
            hi, lo = split(merged_ref[:, start + at : start + at + width])
            total = dot(turned_ref[...], hi)
            out_ref[at : at + width, :] = (total[:rank] + total[rank:] + dot(turned_ref[:rank, :], lo)).T

    return pl.pallas_call(
        body,
        in_specs=[pl.BlockSpec(memory_space=pltpu.VMEM)] * 2,
        out_shape=jax.ShapeDtypeStruct((span, rank), F32),
        name="right",
        **params(6 * rows * span * rank),
    )(merged, turned)


def invert_base(block):
    size = block.shape[0]
    rows = [block[8 * g : 8 * g + 8, :] for g in range(size // 8)]
    lane = lax.broadcasted_iota(jnp.int32, (8, size), 1)
    sub = lax.broadcasted_iota(jnp.int32, (8, size), 0)

    def spread(value):
        return jnp.broadcast_to(value, (8, size))

    for start in range(0, size, 4):
        home, offset = divmod(start, 8)
        inverses, pivots, factors = [], [], {}
        for g in range(home, size // 8):
            columns = [spread(rows[g][:, start + t : start + t + 1]) for t in range(4)]
            row = rows[g]
            for t in range(4):
                s = offset + t
                if g == home:
                    inverse = 1.0 / columns[t][s : s + 1, :]
                    inverses.append(spread(inverse))
                    pivots.append(spread(row[s : s + 1, :] * inverse))
                    for u in range(t + 1, 4):
                        factors[t, u] = spread(columns[u][s : s + 1, :] * inverse)
                below = sub > s
                for u in range(t + 1, 4):
                    new = columns[u] - columns[t] * factors[t, u]
                    columns[u] = jnp.where(below, new, columns[u]) if g == home else new
                new = jnp.where(lane == start + t, -columns[t] * inverses[t], row - columns[t] * pivots[t])
                row = jnp.where(below, new, row) if g == home else new
            rows[g] = row
    out = []
    for g in range(size // 8):
        diagonal = lane == sub + 8 * g
        found = jnp.sum(jnp.where(diagonal, rows[g], 0.0), axis=1, keepdims=True)
        unit = jnp.where(lane < sub + 8 * g, rows[g], jnp.where(diagonal, 1.0, 0.0))
        out.append(unit * (1.0 / jnp.sqrt(found)))
    return jnp.concatenate(out, axis=0)


def full_dot(a, b, dims=NN):
    return lax.dot_general(a, b, dims, precision=HIGH, preferred_element_type=F32)


def invert_factor(gram):
    size = gram.shape[0]
    if size <= LANES:
        return invert_base(gram)
    half = size // 2
    first = invert_factor(gram[:half, :half])
    below = full_dot(gram[half:, :half], first, NT)
    second = invert_factor(gram[half:, half:] - full_dot(below, below, NT))
    corner = -full_dot(second, full_dot(below, first))
    top = jnp.concatenate([first, jnp.zeros((half, size - half), F32)], axis=1)
    return jnp.concatenate([top, jnp.concatenate([corner, second], axis=1)], axis=0)


def ortho_kernel(gram, projected, root):
    rows, rank = projected.shape

    def body(gram_ref, proj_ref, inv_ref, left_ref, wide_ref):
        inverse = invert_factor(gram_ref[...])
        inv_ref[...] = inverse
        i_hi, i_lo = split(inverse)
        ortho = dot(joined3(split(proj_ref[...])), jnp.concatenate([i_hi, i_hi, i_lo], axis=1), NT)
        left_ref[...] = ortho * root
        wide_ref[...] = joined3(split(ortho))

    return pl.pallas_call(
        body,
        out_shape=[
            jax.ShapeDtypeStruct((rank, rank), F32),
            jax.ShapeDtypeStruct((rows, rank), F32),
            jax.ShapeDtypeStruct((rows, 3 * rank), BF16),
        ],
        name="ortho",
        **params(40 * 10**9),
    )(gram, projected)


def coeff_kernel(right, inverse):
    rows, rank = right.shape

    def body(right_ref, inv_ref, out_ref, sq_ref):
        i_hi, i_lo = split(inv_ref[...])
        coeffs = dot(joined3(split(right_ref[...])), jnp.concatenate([i_hi, i_hi, i_lo], axis=1), NT)
        out_ref[...] = coeffs
        sq_ref[...] = jnp.sum(coeffs * coeffs, axis=0, keepdims=True)

    return pl.pallas_call(
        body,
        out_shape=[jax.ShapeDtypeStruct((rows, rank), F32), jax.ShapeDtypeStruct((1, rank), F32)],
        name="coeff",
        **params(6 * rows * rank * rank),
    )(right, inverse)


def update_kernel(merged, wide_ortho, coeffs, start, earlier):
    rows, cols = merged.shape
    span, rank = coeffs.shape
    wide = min(WIDE, span)
    first, steps = start // wide, pl.cdiv(span, wide)
    last = span - (steps - 1) * wide

    def body(ortho_ref, merged_ref, coeff_ref, *rest):
        out_ref = rest[-1]
        step = pl.program_id(0)

        def block(width):
            c_hi, c_lo = split(coeff_ref[:width, :] * -0.5)
            fix = dot(ortho_ref[...], jnp.concatenate([c_hi, c_hi, c_lo], axis=1), NT)
            at = pl.multiple_of((first + step) * wide, wide)
            out_ref[:, :width] = merged_ref[:, pl.ds(at, width)] + fix

        if last == wide:
            block(wide)
        else:
            pl.when(step < steps - 1)(lambda: block(wide))
            pl.when(step == steps - 1)(lambda: block(last))

    more = [] if earlier is None else [earlier]
    return pl.pallas_call(
        body,
        grid=(steps,),
        in_specs=[
            pl.BlockSpec((rows, 3 * rank), lambda j: (0, 0)),
            pl.BlockSpec(memory_space=pltpu.VMEM),
            pl.BlockSpec((wide, rank), lambda j: (j, 0)),
        ]
        + [pl.BlockSpec(memory_space=pl.ANY) for _ in more],
        out_specs=pl.BlockSpec((rows, wide), lambda j: (0, first + j)),
        out_shape=jax.ShapeDtypeStruct((rows, cols), F32),
        input_output_aliases={3: 0} if more else {},
        name="update",
        **params(6 * rows * span * rank),
    )(wide_ortho, merged, coeffs, *more)


def swap(x, axis, size, bit):
    return lax.ppermute(x, axis, [(i, i ^ (1 << bit)) for i in range(size)])


def bits_of(size):
    bits = size.bit_length() - 1
    return bits if size == 1 << bits else None


def keep_and_send(x, mine):
    half = x.shape[0] // 2
    keep = lax.dynamic_slice(x, (mine[half], mine[0]), (half, x.shape[1]), allow_negative_indices=False)
    send = lax.dynamic_slice(x, (mine[-half], mine[0]), (half, x.shape[1]), allow_negative_indices=False)
    return keep, send


def join(own, other, mine):
    return jnp.where(mine["low"], jnp.concatenate([own, other], 0), jnp.concatenate([other, own], 0))


def bit_table(axis, bit, halves):
    mine = (lax.axis_index(axis) >> bit) & 1
    table = {0: jnp.zeros((), jnp.int32), "low": mine == 0}
    for half in halves:
        table[half] = mine * half
        table[-half] = (1 - mine) * half
    return table


def reduce_all(x, axis, size, halved, tables):
    bits = bits_of(size)
    if bits is None or x.shape[0] % (1 << len(halved)):
        return lax.psum(x, axis)
    for bit in halved:
        keep, send = keep_and_send(x, tables[axis, bit])
        x = keep + swap(send, axis, size, bit)
    for bit in range(bits):
        if bit not in halved:
            x = x + swap(x, axis, size, bit)
    for bit in reversed(halved):
        x = join(x, swap(x, axis, size, bit), tables[axis, bit])
    return x


def solution(mesh):
    n_row, n_col = mesh.shape["row"], mesh.shape["col"]
    col_halved = list(range((bits_of(n_col) or 0) - 1))

    def spans_of(cols):
        return [2 * WIDE, 3 * WIDE, cols - 5 * WIDE] if cols > 6 * WIDE else [cols]

    def shards(momentum, activations, out_grads, basis):
        rows, cols = momentum.shape
        spans = spans_of(cols)
        rank = basis.shape[1]
        tables = {("col", b): bit_table("col", b, [rows // 4 >> i for i in range(len(col_halved))]) for b in col_halved}
        tables["row", 0] = bit_table("row", 0, sorted({s // 2 for s in [rank, *spans]}))
        keys = [(t, k) for t in tables for k in tables[t]]
        momentum, *flat = lax.optimization_barrier((momentum, *[tables[t][k] for t, k in keys]))
        for (t, k), value in zip(keys, flat):
            tables[t][k] = value
        merged, *parts = front_kernel(momentum, activations, out_grads, basis, 2)
        parts = [reduce_all(p, "col", n_col, col_halved, tables) for p in parts]
        projected = jnp.concatenate(parts, axis=0)
        gram_part, turned = gram_kernel(projected)
        gram = reduce_all(gram_part, "row", n_row, [0], tables)
        rights = []
        for k, span in enumerate(spans):
            part = right_kernel(merged, turned, sum(spans[:k]), span)
            rights.append(reduce_all(part, "row", n_row, [0], tables))
        inverse, left_basis, wide_ortho = ortho_kernel(gram, projected, math.sqrt(rows * n_row))
        pairs = [coeff_kernel(r, inverse) for r in rights]
        coeffs = [c for c, _ in pairs]
        squares = reduce_all(sum(s for _, s in pairs), "col", n_col, [], tables)
        new_momentum = None
        for k, c in enumerate(coeffs):
            new_momentum = update_kernel(merged, wide_ortho, c, sum(spans[:k]), new_momentum)
        inv_norm = lax.rsqrt(squares / (cols * n_col) + EPS)
        new_basis = jnp.concatenate([c * inv_norm for c in coeffs], axis=0)
        return new_momentum, left_basis, new_basis

    return jax.shard_map(
        shards,
        mesh=mesh,
        in_specs=(P("row", "col"), P(None, "row"), P(None, "col"), P("col", None)),
        out_specs=(P("row", "col"), P("row", None), P("col", None)),
        check_vma=False,
    )
```
